512 devices in a mesh: parts: 2 (over y), blk: 16 (over z), sub: 8 (over x), rep: 2 (over core).
Axes of the slice: x: 8, y: 2, z: 16, core: 2. Of those that a mesh axis runs over, the one named last changes fastest.
The devices are a block of a 8x16x16 slice.
Arguments:
- queries: bfloat16 [2048, 32, 128], P(('parts', 'blk', 'sub', 'rep')), parts along dimension 0, may hold values from -1.5 to 1.5
- passages: bfloat16 [2048, 128, 128], P(('parts', 'blk')), parts along dimension 0, may hold values from -1.5 to 1.5
- lengths: int32 [2048], P(('parts', 'blk')), parts along dimension 0, may hold values from 8 to 128
- slot_of: int32 [2048], P('parts'), parts along dimension 0, may hold values from 0 to 1023, each once
- candidates: int32 [2048, 256], P(('parts', 'blk', 'sub', 'rep')), parts along dimension 0, may hold values from 0 to 1023
Outputs:
- score: float32 [2048, 256], P(('parts', 'blk', 'sub', 'rep')), parts along dimension 0
- top: float32 [2048, 10], P(('parts', 'blk', 'sub', 'rep')), parts along dimension 0
The draws below stay inside these ranges and needn't reach their ends.
There are 2 independent parts, one for each index of `parts`. The reference program is written for one: setup_inputs(seed, part) draws one part's arguments, and reference() takes and returns one part's arrays. A program takes and returns all parts, laid end to end along the dimension named above; each array names one. Nothing has to cross between parts.
Inputs may be any that keep to these rules, and one draw needn't show every extreme that they name: `slot_of`: a permutation; storage row r lies on the blk index r // 64. `candidates`: passage ids, repeats allowed. `lengths`: the live slots of a row are its first ones.
All inputs are finite; a program needn't handle non-finite values.
Results may differ from the reference program's by a relative error of at most 0.0003.
Values may be sent and summed in bfloat16 or wider, within the bound.
A program may use at most 64 MiB of HBM per device.

```python
import math
import jax
import jax.numpy as jnp
import numpy as np
from jax import lax

DIM = 128
QT = 32
LP = 128
K = 256
TOPN = 10
NQ = 1024
NP = 1024


def set_ends(drawn, stream_key, low, high):
    extent = drawn.shape
    index_at = [jax.random.randint(jax.random.fold_in(stream_key, axis), (), 0, extent[axis]) for axis in range(len(extent))]
    drawn = drawn.at[tuple(index_at)].set(low)
    longest = extent.index(max(extent))
    index_at[longest] = (index_at[longest] + 1) % extent[longest]
    return drawn.at[tuple(index_at)].set(high)


def steps_of(own_key, extent, split, least, high):
    loudness, own = 1.0, jax.random.fold_in(own_key, 6)
    for axis_at, shards_of in split:
        heights = jnp.exp(jax.random.uniform(jax.random.fold_in(own, axis_at), (shards_of,), jnp.float32, least / len(split), high / len(split)))
        loudness = loudness * jnp.repeat(heights, extent[axis_at] // shards_of).reshape([-1 if axis == axis_at else 1 for axis in range(len(extent))])
    return loudness


def cumulative_ranks(count, skew):
    loads = [(1 << 20) // math.isqrt(grade ** skew) + 1 for grade in range(1, count + 1)]
    scale = 1 + sum(loads) // (1 << 30)
    return np.cumsum(np.array([max(1, weight // scale) for weight in loads]))


def skewed_ids(own_key, extent, number_of, lean):
    grid = cumulative_ranks(number_of, lean)
    ticket = jax.random.randint(jax.random.fold_in(own_key, 1), extent, 0, int(grid[number_of - 1]))
    grade = jnp.searchsorted(jnp.asarray(grid, jnp.int32), ticket, side="right")
    return jax.random.permutation(jax.random.fold_in(own_key, 2), number_of)[grade].astype(jnp.int32)


def noise(key, extent, scale, bound, pieces=(), kind=jnp.bfloat16):
    entries = jax.random.normal(key, extent, jnp.float32) * scale
    if len(pieces) > 0:
        entries = steps_of(key, extent, pieces, -0.22, 0.18) * entries
    return jnp.clip(entries, min=-bound, max=bound).astype(kind)


def setup_inputs(seed: int = 0, part: int = 0) -> dict:
    key_of = jax.random.split(jax.random.key(seed), 6)
    part_splits = jax.random.split(jax.random.fold_in(key_of[5], part), 6)
    return {
        "queries": noise(part_splits[0], (NQ, QT, DIM), 0.25, 1.5, ((0, 256),)),
        "passages": noise(part_splits[1], (NP, LP, DIM), 0.25, 1.5, ((0, 16),)),
        "lengths": set_ends(jax.random.randint(part_splits[2], (NP,), 8, LP + 1), jax.random.fold_in(part_splits[2], 1), 8, LP).astype(jnp.int32),
        "slot_of": jax.random.permutation(part_splits[3], NP).astype(jnp.int32),
        "candidates": set_ends(skewed_ids(part_splits[4], (NQ, K), NP, 2), jax.random.fold_in(part_splits[4], 3), 0, NP - 1).astype(jnp.int32),
    }


def reference(queries, passages, lengths, slot_of, candidates):
    query_count = queries.shape[0]
    passage_count = passages.shape[0]
    flat = queries.reshape(query_count * QT, DIM)
    blocks = passages.reshape(passage_count // 8, 8 * LP, DIM)
    spans = lengths.reshape(passage_count // 8, 8)

    def one_block(pair):
        piece, live_count = pair
        similar = jnp.dot(flat, piece.T, preferred_element_type=jnp.float32)
        similar = similar.reshape(query_count * QT, 8, LP)
        live = jnp.arange(LP, dtype=jnp.int32)[None, :] < live_count[:, None]
        best = jnp.max(jnp.where(live[None], similar, -1e30), axis=2)
        return jnp.sum(best.reshape(query_count, QT, 8), axis=1) / QT

    table = lax.map(one_block, (blocks, spans))
    table = jnp.transpose(table, (1, 0, 2)).reshape(query_count, passage_count)
    storage_rows = jnp.take(slot_of, candidates, axis=0).astype(jnp.int32)
    score = jnp.take_along_axis(table, storage_rows, axis=1)
    top = lax.top_k(score, TOPN)[0]
    return score, top
```

```python
import functools

import jax
import jax.numpy as jnp
from jax import lax
from jax.experimental import pallas as pl
from jax.experimental.pallas import tpu as pltpu
from jax.sharding import PartitionSpec as P

MESH = pl.DeviceIdType.MESH
TOPN = 10
F32 = jnp.float32
BF16 = jnp.bfloat16


def slot(side, d):
    return 2 * d - 1 if side == 1 else 2 * d


def gather_rows(table, row_of, lane_of):
    found = jnp.zeros(row_of.shape, table.dtype)
    for row in range(table.shape[0]):
        line = jnp.broadcast_to(table[row : row + 1, :], row_of.shape)
        picked = jnp.take_along_axis(line, lane_of, axis=1, mode="promise_in_bounds")
        found = jnp.where(row_of == row, picked, found)
    return found


def kernel(
    n, q_ref, p_hbm, len_ref, slot_ref, cand_ref, score_ref, top_ref,
    own, held, stored, weights, best, outgoing, table, load_sem, send_sem, recv_sem, back_send, back_recv,
):
    me = lax.axis_index("blk")
    half = n // 2
    count, span, width = p_hbm.shape
    pairs = count // 2
    queries_here, tokens = q_ref.shape[0], q_ref.shape[1]
    cols = queries_here * tokens

    def at(shift):
        return {"blk": lax.rem(me + shift + n, n)}

    loads = []
    for side in range(2):
        load = pltpu.make_async_copy(
            p_hbm.at[pl.ds(side * pairs, pairs)],
            stored.at[:, :, pl.ds(side * width, width)],
            load_sem.at[side],
        )
        load.start()
        loads.append(load)

    barrier = pltpu.get_barrier_semaphore()
    for d in (4, 2, 1):
        for side in (1, -1):
            pl.semaphore_signal(barrier, inc=1, device_id=at(side * d), device_id_type=MESH)

    flat = q_ref[...].reshape(cols, width).astype(F32)
    own[...] = flat.T.astype(BF16)
    weights[...] = jnp.zeros_like(weights)

    pl.semaphore_wait(barrier, 6)

    started = []

    def send(side, hop, source, d):
        src = own if source == 0 else held.at[slot(side, source)]
        if d == half:
            part = pl.ds(0 if side == 1 else width // 2, width // 2)
            src = src.at[part]
            dst = held.at[n - 1].at[part]
            sem = n - 1 if side == 1 else n
        else:
            dst = held.at[slot(side, d)]
            sem = slot(side, d)
        copy = pltpu.make_async_remote_copy(
            src_ref=src, dst_ref=dst, send_sem=send_sem.at[sem], recv_sem=recv_sem.at[sem],
            device_id=at(side * hop), device_id_type=MESH,
        )
        copy.start()
        started.append(copy)

    def arrived(side, d):
        started_like[(side, d)].wait_recv()

    started_like = {}

    def send_both(hop, source, d):
        for side in (1, -1):
            send(side, hop, source, d)
            started_like[(side, d)] = started[-1]

    def wait_both(d):
        for side in (1, -1):
            arrived(side, d)

    send_both(4, 0, 4)
    send_both(2, 0, 2)
    send_both(1, 0, 1)

    cand = jnp.concatenate(
        [cand_ref[q : q + 1, h * 128 : (h + 1) * 128] for q in range(queries_here) for h in range(2)], axis=0
    )
    rows = gather_rows(slot_ref[...], cand // 128, cand % 128)
    query_of = lax.broadcasted_iota(jnp.int32, rows.shape, 0) // 2

    for load in loads:
        load.wait()

    def keep_live(pair, _):
        for side in range(2):
            lanes = pl.ds(side * width, width)
            piece = stored[pair, :, lanes].astype(F32)
            live = lax.broadcasted_iota(jnp.int32, piece.shape, 0) < len_ref[pair + side * pairs]
            stored[pair, :, lanes] = jnp.where(live, piece, piece[0:1, :]).astype(BF16)
        return 0

    lax.fori_loop(0, pairs, keep_live, 0)

    r_at = lax.broadcasted_iota(jnp.int32, (2 * cols, cols), 0) % cols
    c_at = lax.broadcasted_iota(jnp.int32, (2 * cols, cols), 1)
    ones_of = jnp.where(r_at // tokens == c_at // tokens, 1.0 / tokens, 0.0).astype(BF16)
    mine = (
        lax.broadcasted_iota(jnp.int32, (pairs, cols), 0) == lax.broadcasted_iota(jnp.int32, (pairs, cols), 1) % tokens
    )

    def score_block(query_cols):
        weights[0:width, 0:cols] = query_cols
        weights[width : 2 * width, cols : 2 * cols] = query_cols
        rhs = weights[...]
        for pair in range(pairs):
            similar = jnp.dot(stored[pair], rhs, preferred_element_type=F32)
            best[pair : pair + 1, :] = jnp.max(similar, axis=0, keepdims=True)
        lines = []
        for side in range(2):
            value = best[:, side * cols : (side + 1) * cols]
            high = value.astype(BF16)
            low = (value - high.astype(F32)).astype(BF16)
            summed = jnp.dot(jnp.concatenate([high, low], axis=1), ones_of, preferred_element_type=F32)
            lines.append(jnp.sum(jnp.where(mine, summed, 0.0), axis=0, keepdims=True))
        return jnp.concatenate(lines, axis=0)

    def back(s):
        d = (s + 1) // 2
        side = 2 * lax.rem(s, 2) - 1
        return pltpu.make_async_remote_copy(
            src_ref=outgoing.at[s], dst_ref=table.at[me], send_sem=back_send.at[s], recv_sem=back_recv.at[s],
            device_id=at(-side * d), device_id_type=MESH,
        )

    def score_slots(low, high):
        def one(s, _):
            outgoing[s] = score_block(held[s])
            back(s).start()
            return 0

        lax.fori_loop(low, high, one, 0)

    table[me] = score_block(own[...])

    wait_both(2)
    send_both(1, 2, 3)
    wait_both(1)
    score_slots(1, 3)
    wait_both(4)
    send_both(4, 4, 8)
    send_both(2, 4, 6)
    send_both(1, 4, 5)
    wait_both(3)
    score_slots(3, 7)
    wait_both(6)
    send_both(1, 6, 7)
    wait_both(5)
    score_slots(7, 13)
    wait_both(8)
    wait_both(7)
    score_slots(13, n)

    def land(s, _):
        back(s).wait_recv()
        return 0

    lax.fori_loop(1, n, land, 0)

    lines = table[...].reshape(2 * n, cols)
    score = gather_rows(lines, rows // tokens, query_of * tokens + rows % tokens)
    for q in range(queries_here):
        for h in range(2):
            score_ref[q : q + 1, h * 128 : (h + 1) * 128] = score[2 * q + h : 2 * q + h + 1, :]

    down = score.T
    j_at = lax.broadcasted_iota(jnp.int32, (128, 128), 0)
    k_at = lax.broadcasted_iota(jnp.int32, (128, 128), 1)
    place = lax.broadcasted_iota(jnp.int32, (16, 128), 0).astype(F32)
    spot = lax.broadcasted_iota(jnp.int32, (16, 128), 0) == lax.broadcasted_iota(jnp.int32, (16, 128), 1)
    for q in range(queries_here):
        total = jnp.zeros((16, 1), F32)
        for kh in range(2):
            k_val = score[2 * q + kh : 2 * q + kh + 1, :]
            rank = jnp.zeros((1, 128), F32)
            for jh in range(2):
                j_val = down[:, 2 * q + jh : 2 * q + jh + 1]
                if jh < kh:
                    ahead = j_val >= k_val
                elif jh > kh:
                    ahead = j_val > k_val
                else:
                    ahead = (j_val > k_val) | ((j_val == k_val) & (j_at < k_at))
                rank = rank + jnp.sum(jnp.where(ahead, 1.0, 0.0), axis=0, keepdims=True)
            total = total + jnp.sum(jnp.where(rank == place, k_val, 0.0), axis=1, keepdims=True)
        line = jnp.sum(jnp.where(spot, total, 0.0), axis=0, keepdims=True)
        top_ref[q : q + 1, :] = line[:, 0:TOPN]

    for copy in started:
        copy.wait_send()

    def sent(s, _):
        back(s).wait_send()
        return 0

    lax.fori_loop(1, n, sent, 0)


def shards(n, queries, passages, lengths, slot_of, candidates):
    queries_here, tokens, width = queries.shape
    count, span, _ = passages.shape
    cols = queries_here * tokens
    vmem = pl.BlockSpec(memory_space=pltpu.VMEM)
    return pl.pallas_call(
        functools.partial(kernel, n),
        out_shape=(
            jax.ShapeDtypeStruct(candidates.shape, F32),
            jax.ShapeDtypeStruct((queries_here, TOPN), F32),
        ),
        in_specs=[
            vmem,
            pl.BlockSpec(memory_space=pl.ANY),
            pl.BlockSpec(memory_space=pltpu.SMEM),
            vmem,
            vmem,
        ],
        out_specs=(vmem, vmem),
        scratch_shapes=[
            pltpu.VMEM((width, cols), BF16),
            pltpu.VMEM((n, width, cols), BF16),
            pltpu.VMEM((count // 2, span, 2 * width), BF16),
            pltpu.VMEM((2 * width, 2 * cols), BF16),
            pltpu.VMEM((count // 2, 2 * cols), F32),
            pltpu.VMEM((n, 2, cols), F32),
            pltpu.VMEM((n, 2, cols), F32),
            pltpu.SemaphoreType.DMA((2,)),
            pltpu.SemaphoreType.DMA((n + 1,)),
            pltpu.SemaphoreType.DMA((n + 1,)),
            pltpu.SemaphoreType.DMA((n,)),
            pltpu.SemaphoreType.DMA((n,)),
        ],
        compiler_params=pltpu.CompilerParams(collective_id=0, has_side_effects=True),
    )(queries, passages, lengths, slot_of.reshape(-1, 128), candidates)


def solution(mesh):
    return jax.shard_map(
        functools.partial(shards, mesh.shape["blk"]),
        mesh=mesh,
        in_specs=(
            P(("parts", "blk", "sub", "rep"), None, None),
            P(("parts", "blk"), None, None),
            P(("parts", "blk")),
            P("parts"),
            P(("parts", "blk", "sub", "rep"), None),
        ),
        out_specs=(
            P(("parts", "blk", "sub", "rep"), None),
            P(("parts", "blk", "sub", "rep"), None),
        ),
        check_vma=False,
    )
```

```python
import functools

import jax
import jax.numpy as jnp
from jax import lax
from jax.experimental import pallas as pl
from jax.experimental.pallas import tpu as pltpu
from jax.sharding import PartitionSpec as P

MESH = pl.DeviceIdType.MESH
TOPN = 10
F32 = jnp.float32
BF16 = jnp.bfloat16


def gather_rows(table, row_of, lane_of):
    found = jnp.zeros(row_of.shape, table.dtype)
    for row in range(table.shape[0]):
        line = jnp.broadcast_to(table[row : row + 1, :], row_of.shape)
        picked = jnp.take_along_axis(line, lane_of, axis=1, mode="promise_in_bounds")
        found = jnp.where(row_of == row, picked, found)
    return found


def kernel(
    n, q_ref, p_hbm, len_ref, slot_ref, cand_ref, score_ref, top_ref,
    own, held, stored, weights, best, outgoing, table, load_sem, up_send, down_send, recv_sem, back_send, back_recv,
):
    me = lax.axis_index("blk")
    count, span, width = p_hbm.shape
    pairs = count // 2
    queries_here, tokens = q_ref.shape[0], q_ref.shape[1]
    cols = queries_here * tokens

    last = n - 1

    loads = []
    for side in range(2):
        load = pltpu.make_async_copy(
            p_hbm.at[pl.ds(side * pairs, pairs)],
            stored.at[:, :, pl.ds(side * width, width)],
            load_sem.at[side],
        )
        load.start()
        loads.append(load)

    barrier = pltpu.get_barrier_semaphore()
    pl.semaphore_signal(barrier, inc=1, device_id={"blk": lax.rem(me + last, n)}, device_id_type=MESH)

    flat = q_ref[...].reshape(cols, width).astype(F32)
    own[...] = flat.T.astype(BF16)
    weights[...] = jnp.zeros_like(weights)

    def climb(k, src):
        return pltpu.make_async_remote_copy(
            src_ref=src, dst_ref=held.at[k], send_sem=up_send.at[k], recv_sem=recv_sem.at[k],
            device_id={"blk": lax.rem(me + 1, n)}, device_id_type=MESH,
        )

    def direct(k):
        return pltpu.make_async_remote_copy(
            src_ref=own, dst_ref=held.at[me], send_sem=down_send.at[k], recv_sem=recv_sem.at[me],
            device_id={"blk": k}, device_id_type=MESH,
        )

    def back(k):
        return pltpu.make_async_remote_copy(
            src_ref=outgoing.at[k], dst_ref=table.at[me], send_sem=back_send.at[k], recv_sem=back_recv.at[me],
            device_id={"blk": k}, device_id_type=MESH,
        )

    def loop(low, high, step):
        def one(k, _):
            step(k)
            return 0

        lax.fori_loop(low, high, one, 0)

    cand = jnp.concatenate(
        [cand_ref[q : q + 1, h * 128 : (h + 1) * 128] for q in range(queries_here) for h in range(2)], axis=0
    )
    rows = gather_rows(slot_ref[...], cand // 128, cand % 128)
    query_of = lax.broadcasted_iota(jnp.int32, rows.shape, 0) // 2

    for load in loads:
        load.wait()

    def keep_live(pair, _):
        for side in range(2):
            lanes = pl.ds(side * width, width)
            piece = stored[pair, :, lanes].astype(F32)
            live = lax.broadcasted_iota(jnp.int32, piece.shape, 0) < len_ref[pair + side * pairs]
            stored[pair, :, lanes] = jnp.where(live, piece, piece[0:1, :]).astype(BF16)
        return 0

    lax.fori_loop(0, pairs, keep_live, 0)

    r_at = lax.broadcasted_iota(jnp.int32, (2 * cols, cols), 0) % cols
    c_at = lax.broadcasted_iota(jnp.int32, (2 * cols, cols), 1)
    ones_of = jnp.where(r_at // tokens == c_at // tokens, 1.0 / tokens, 0.0).astype(BF16)
    mine = (
        lax.broadcasted_iota(jnp.int32, (pairs, cols), 0) == lax.broadcasted_iota(jnp.int32, (pairs, cols), 1) % tokens
    )

    def score_block(query_cols):
        weights[0:width, 0:cols] = query_cols
        weights[width : 2 * width, cols : 2 * cols] = query_cols
        rhs = weights[...]
        for pair in range(pairs):
            similar = jnp.dot(stored[pair], rhs, preferred_element_type=F32)
            best[pair : pair + 1, :] = jnp.max(similar, axis=0, keepdims=True)
        lines = []
        for side in range(2):
            value = best[:, side * cols : (side + 1) * cols]
            high = value.astype(BF16)
            low = (value - high.astype(F32)).astype(BF16)
            summed = jnp.dot(jnp.concatenate([high, low], axis=1), ones_of, preferred_element_type=F32)
            lines.append(jnp.sum(jnp.where(mine, summed, 0.0), axis=0, keepdims=True))
        return jnp.concatenate(lines, axis=0)

    def arrived(k):
        pltpu.make_async_remote_copy(
            src_ref=own, dst_ref=held.at[k], send_sem=up_send.at[k], recv_sem=recv_sem.at[k],
            device_id={"blk": me}, device_id_type=MESH,
        ).wait_recv()

    def landed(k):
        pltpu.make_async_remote_copy(
            src_ref=outgoing.at[k], dst_ref=table.at[k], send_sem=back_send.at[k], recv_sem=back_recv.at[k],
            device_id={"blk": me}, device_id_type=MESH,
        ).wait_recv()

    table[me] = score_block(own[...])

    pl.semaphore_wait(barrier, 1)

    def answer(k):
        outgoing[k] = score_block(held[k])
        back(k).start()

    def from_below(k):
        arrived(k)

        @pl.when(me < last)
        def _():
            climb(k, held.at[k]).start()

        answer(k)

    def from_above(k):
        arrived(k)
        answer(k)

    loop(0, me, from_below)

    @pl.when(me < last)
    def _():
        climb(me, own).start()

    loop(0, me, lambda k: direct(k).start())
    loop(me + 1, n, from_above)
    loop(0, me, landed)
    loop(me + 1, n, landed)

    lines = table[...].reshape(2 * n, cols)
    score = gather_rows(lines, rows // tokens, query_of * tokens + rows % tokens)
    for q in range(queries_here):
        for h in range(2):
            score_ref[q : q + 1, h * 128 : (h + 1) * 128] = score[2 * q + h : 2 * q + h + 1, :]

    down = score.T
    j_at = lax.broadcasted_iota(jnp.int32, (128, 128), 0)
    k_at = lax.broadcasted_iota(jnp.int32, (128, 128), 1)
    place = lax.broadcasted_iota(jnp.int32, (16, 128), 0).astype(F32)
    spot = lax.broadcasted_iota(jnp.int32, (16, 128), 0) == lax.broadcasted_iota(jnp.int32, (16, 128), 1)
    for q in range(queries_here):
        total = jnp.zeros((16, 1), F32)
        for kh in range(2):
            k_val = score[2 * q + kh : 2 * q + kh + 1, :]
            rank = jnp.zeros((1, 128), F32)
            for jh in range(2):
                j_val = down[:, 2 * q + jh : 2 * q + jh + 1]
                if jh < kh:
                    ahead = j_val >= k_val
                elif jh > kh:
                    ahead = j_val > k_val
                else:
                    ahead = (j_val > k_val) | ((j_val == k_val) & (j_at < k_at))
                rank = rank + jnp.sum(jnp.where(ahead, 1.0, 0.0), axis=0, keepdims=True)
            total = total + jnp.sum(jnp.where(rank == place, k_val, 0.0), axis=1, keepdims=True)
        line = jnp.sum(jnp.where(spot, total, 0.0), axis=0, keepdims=True)
        top_ref[q : q + 1, :] = line[:, 0:TOPN]

    @pl.when(me < last)
    def _():
        loop(0, me, lambda k: climb(k, held.at[k]).wait_send())
        climb(me, own).wait_send()

    loop(0, me, lambda k: direct(k).wait_send())
    loop(0, me, lambda k: back(k).wait_send())
    loop(me + 1, n, lambda k: back(k).wait_send())


def shards(n, queries, passages, lengths, slot_of, candidates):
    queries_here, tokens, width = queries.shape
    count, span, _ = passages.shape
    cols = queries_here * tokens
    vmem = pl.BlockSpec(memory_space=pltpu.VMEM)
    return pl.pallas_call(
        functools.partial(kernel, n),
        out_shape=(
            jax.ShapeDtypeStruct(candidates.shape, F32),
            jax.ShapeDtypeStruct((queries_here, TOPN), F32),
        ),
        in_specs=[
            vmem,
            pl.BlockSpec(memory_space=pl.ANY),
            pl.BlockSpec(memory_space=pltpu.SMEM),
            vmem,
            vmem,
        ],
        out_specs=(vmem, vmem),
        scratch_shapes=[
            pltpu.VMEM((width, cols), BF16),
            pltpu.VMEM((n, width, cols), BF16),
            pltpu.VMEM((count // 2, span, 2 * width), BF16),
            pltpu.VMEM((2 * width, 2 * cols), BF16),
            pltpu.VMEM((count // 2, 2 * cols), F32),
            pltpu.VMEM((n, 2, cols), F32),
            pltpu.VMEM((n, 2, cols), F32),
            pltpu.SemaphoreType.DMA((2,)),
            pltpu.SemaphoreType.DMA((n,)),
            pltpu.SemaphoreType.DMA((n,)),
            pltpu.SemaphoreType.DMA((n,)),
            pltpu.SemaphoreType.DMA((n,)),
            pltpu.SemaphoreType.DMA((n,)),
        ],
        compiler_params=pltpu.CompilerParams(collective_id=0, has_side_effects=True),
    )(queries, passages, lengths, slot_of.reshape(-1, 128), candidates)


def solution(mesh):
    return jax.shard_map(
        functools.partial(shards, mesh.shape["blk"]),
        mesh=mesh,
        in_specs=(
            P(("parts", "blk", "sub", "rep"), None, None),
            P(("parts", "blk"), None, None),
            P(("parts", "blk")),
            P("parts"),
            P(("parts", "blk", "sub", "rep"), None),
        ),
        out_specs=(
            P(("parts", "blk", "sub", "rep"), None),
            P(("parts", "blk", "sub", "rep"), None),
        ),
        check_vma=False,
    )
```

```python
import functools

import jax
import jax.numpy as jnp
from jax import lax
from jax.experimental import pallas as pl
from jax.experimental.pallas import tpu as pltpu
from jax.sharding import PartitionSpec as P

MESH = pl.DeviceIdType.MESH
TOPN = 10
HOT = 4
F32 = jnp.float32
BF16 = jnp.bfloat16


def order(z, n, hot):
    last = n - 1
    if z == 0:
        return list(range(1, n))
    if z < hot:
        rest = [k for k in range(1, n) if k != z]
        return rest[:9] + [0] + rest[9:]
    sources = list(range(hot, z))
    if z > n // 2:
        for k in range(hot):
            sources.insert(min(1 + 2 * (k + last - z), len(sources)), k)
        return sources + list(range(z + 1, n))
    sources += list(range(1, hot)) + list(range(z + 1, n))
    return sources[:9] + [0] + sources[9:]


def picked_by(table, me):
    words = []
    for start in range(0, len(table[0]), 5):
        word = jnp.int32(0)
        for z, line in enumerate(table):
            packed = sum(value * 32**i for i, value in enumerate(line[start : start + 5]))
            word = jnp.where(me == z, packed, word)
        words.append(word)

    def pick(at):
        word = words[-1]
        for i in range(len(words) - 1):
            word = jnp.where(at // 5 == i, words[i], word)
        return lax.rem(lax.shift_right_logical(word, 5 * lax.rem(at, 5)), 32)

    return pick


def gather_rows(table, row_of, lane_of):
    found = jnp.zeros(row_of.shape, table.dtype)
    for row in range(table.shape[0]):
        line = jnp.broadcast_to(table[row : row + 1, :], row_of.shape)
        picked = jnp.take_along_axis(line, lane_of, axis=1, mode="promise_in_bounds")
        found = jnp.where(row_of == row, picked, found)
    return found


def kernel(
    n, q_ref, p_hbm, len_ref, slot_ref, cand_ref, score_ref, top_ref,
    own, held, stored, weights, best, outgoing, table, load_sem, up_send, down_send, recv_sem, back_send, back_recv, asked,
):
    me = lax.axis_index("blk")
    count, span, width = p_hbm.shape
    pairs = count // 2
    queries_here, tokens = q_ref.shape[0], q_ref.shape[1]
    cols = queries_here * tokens

    last = n - 1
    hot = HOT
    lag = n // 2

    loads = []
    for side in range(2):
        load = pltpu.make_async_copy(
            p_hbm.at[pl.ds(side * pairs, pairs)],
            stored.at[:, :, pl.ds(side * width, width)],
            load_sem.at[side],
        )
        load.start()
        loads.append(load)

    flat = q_ref[...].reshape(cols, width).astype(F32)
    own[...] = flat.T.astype(BF16)
    weights[...] = jnp.zeros_like(weights)

    def climb(k, src):
        return pltpu.make_async_remote_copy(
            src_ref=src, dst_ref=held.at[k], send_sem=up_send.at[k], recv_sem=recv_sem.at[k],
            device_id={"blk": lax.rem(me + 1, n)}, device_id_type=MESH,
        )

    def direct(k):
        return pltpu.make_async_remote_copy(
            src_ref=own, dst_ref=held.at[me], send_sem=down_send.at[k], recv_sem=recv_sem.at[me],
            device_id={"blk": k}, device_id_type=MESH,
        )

    def back(k):
        return pltpu.make_async_remote_copy(
            src_ref=outgoing.at[k], dst_ref=table.at[me], send_sem=back_send.at[k], recv_sem=back_recv.at[me],
            device_id={"blk": k}, device_id_type=MESH,
        )

    def loop(low, high, step):
        def one(k, _):
            step(k)
            return 0

        lax.fori_loop(low, high, one, 0)

    barrier = pltpu.get_barrier_semaphore()

    @pl.when(me > 1)
    def _():
        pl.semaphore_wait(barrier, 1)

    @pl.when(me > 0)
    def _():
        pl.semaphore_signal(barrier, inc=1, device_id={"blk": 0}, device_id_type=MESH)

    @pl.when((me > 0) & (me < last))
    def _():
        pl.semaphore_signal(barrier, inc=1, device_id={"blk": lax.rem(me + 1, n)}, device_id_type=MESH)

    def ask(k):
        pl.semaphore_signal(asked.at[me], inc=1, device_id={"blk": k}, device_id_type=MESH)

    @pl.when(me > hot)
    def _():
        ask(lax.rem(me + last, n))

    loop(1, jnp.minimum(me, hot), ask)

    cand = jnp.concatenate(
        [cand_ref[q : q + 1, h * 128 : (h + 1) * 128] for q in range(queries_here) for h in range(2)], axis=0
    )
    rows = gather_rows(slot_ref[...], cand // 128, cand % 128)
    query_of = lax.broadcasted_iota(jnp.int32, rows.shape, 0) // 2

    for load in loads:
        load.wait()

    def keep_live(pair, _):
        for side in range(2):
            lanes = pl.ds(side * width, width)
            piece = stored[pair, :, lanes].astype(F32)
            live = lax.broadcasted_iota(jnp.int32, piece.shape, 0) < len_ref[pair + side * pairs]
            stored[pair, :, lanes] = jnp.where(live, piece, piece[0:1, :]).astype(BF16)
        return 0

    lax.fori_loop(0, pairs, keep_live, 0)

    r_at = lax.broadcasted_iota(jnp.int32, (2 * cols, cols), 0) % cols
    c_at = lax.broadcasted_iota(jnp.int32, (2 * cols, cols), 1)
    ones_of = jnp.where(r_at // tokens == c_at // tokens, 1.0 / tokens, 0.0).astype(BF16)
    mine = (
        lax.broadcasted_iota(jnp.int32, (pairs, cols), 0) == lax.broadcasted_iota(jnp.int32, (pairs, cols), 1) % tokens
    )

    def score_block(query_cols):
        weights[0:width, 0:cols] = query_cols
        weights[width : 2 * width, cols : 2 * cols] = query_cols
        rhs = weights[...]
        for pair in range(pairs):
            similar = jnp.dot(stored[pair], rhs, preferred_element_type=F32)
            best[pair : pair + 1, :] = jnp.max(similar, axis=0, keepdims=True)
        lines = []
        for side in range(2):
            value = best[:, side * cols : (side + 1) * cols]
            high = value.astype(BF16)
            low = (value - high.astype(F32)).astype(BF16)
            summed = jnp.dot(jnp.concatenate([high, low], axis=1), ones_of, preferred_element_type=F32)
            lines.append(jnp.sum(jnp.where(mine, summed, 0.0), axis=0, keepdims=True))
        return jnp.concatenate(lines, axis=0)

    def arrived(k):
        pltpu.make_async_remote_copy(
            src_ref=own, dst_ref=held.at[k], send_sem=up_send.at[k], recv_sem=recv_sem.at[k],
            device_id={"blk": me}, device_id_type=MESH,
        ).wait_recv()

    def landed(k):
        pltpu.make_async_remote_copy(
            src_ref=outgoing.at[k], dst_ref=table.at[k], send_sem=back_send.at[k], recv_sem=back_recv.at[k],
            device_id={"blk": me}, device_id_type=MESH,
        ).wait_recv()

    table[me] = score_block(own[...])

    source_at = picked_by([order(z, n, hot) for z in range(n)], me)

    def answer(k):
        outgoing[k] = score_block(held[k])
        back(k).start()

    @pl.when(me < hot)
    def _():
        loop(1, me, lambda k: direct(k).start())

        def step(t):
            later = me + 1 + t

            @pl.when(later < n)
            def _():
                @pl.when(me == 0)
                def _():
                    pl.semaphore_wait(barrier, 1)

                @pl.when(me > 0)
                def _():
                    pl.semaphore_wait(asked.at[later], 1)

                direct(later).start()

            @pl.when(t >= lag)
            def _():
                k = source_at(jnp.maximum(t - lag, 0))
                arrived(k)

                @pl.when(k == 0)
                def _():
                    direct(k).start()

                answer(k)

        loop(0, last + lag, step)

    @pl.when(me >= hot)
    def _():
        def step(t):
            k = source_at(t)
            arrived(k)

            @pl.when(k == 0)
            def _():
                direct(k).start()

            @pl.when(me < last)
            def _():
                @pl.when(t == 0)
                def _():
                    pl.semaphore_wait(asked.at[lax.rem(me + 1, n)], 1)

                @pl.when((k >= hot) & (k < me))
                def _():
                    climb(k, held.at[k]).start()

                @pl.when(t == 0)
                def _():
                    climb(me, own).start()

            answer(k)

            @pl.when(t < me - 1)
            def _():
                direct(jnp.where(lax.rem(t, 2) == 0, 1 + t // 2, me - 1 - t // 2)).start()

        loop(0, last, step)

    loop(0, me, landed)
    loop(me + 1, n, landed)

    lines = table[...].reshape(2 * n, cols)
    score = gather_rows(lines, rows // tokens, query_of * tokens + rows % tokens)
    for q in range(queries_here):
        for h in range(2):
            score_ref[q : q + 1, h * 128 : (h + 1) * 128] = score[2 * q + h : 2 * q + h + 1, :]

    down = score.T
    j_at = lax.broadcasted_iota(jnp.int32, (128, 128), 0)
    k_at = lax.broadcasted_iota(jnp.int32, (128, 128), 1)
    place = lax.broadcasted_iota(jnp.int32, (16, 128), 0).astype(F32)
    spot = lax.broadcasted_iota(jnp.int32, (16, 128), 0) == lax.broadcasted_iota(jnp.int32, (16, 128), 1)
    for q in range(queries_here):
        total = jnp.zeros((16, 1), F32)
        for kh in range(2):
            k_val = score[2 * q + kh : 2 * q + kh + 1, :]
            rank = jnp.zeros((1, 128), F32)
            for jh in range(2):
                j_val = down[:, 2 * q + jh : 2 * q + jh + 1]
                if jh < kh:
                    ahead = j_val >= k_val
                elif jh > kh:
                    ahead = j_val > k_val
                else:
                    ahead = (j_val > k_val) | ((j_val == k_val) & (j_at < k_at))
                rank = rank + jnp.sum(jnp.where(ahead, 1.0, 0.0), axis=0, keepdims=True)
            total = total + jnp.sum(jnp.where(rank == place, k_val, 0.0), axis=1, keepdims=True)
        line = jnp.sum(jnp.where(spot, total, 0.0), axis=0, keepdims=True)
        top_ref[q : q + 1, :] = line[:, 0:TOPN]

    @pl.when((me >= hot) & (me < last))
    def _():
        loop(hot, me, lambda k: climb(k, held.at[k]).wait_send())
        climb(me, own).wait_send()

    @pl.when(me < hot)
    def _():
        loop(me + 1, n, lambda k: direct(k).wait_send())

    loop(0, me, lambda k: back(k).wait_send())
    loop(me + 1, n, lambda k: back(k).wait_send())

    @pl.when(me > 0)
    def _():
        direct(jnp.int32(0)).wait_send()

    loop(1, me, lambda k: direct(k).wait_send())


def shards(n, queries, passages, lengths, slot_of, candidates):
    queries_here, tokens, width = queries.shape
    count, span, _ = passages.shape
    cols = queries_here * tokens
    vmem = pl.BlockSpec(memory_space=pltpu.VMEM)
    return pl.pallas_call(
        functools.partial(kernel, n),
        out_shape=(
            jax.ShapeDtypeStruct(candidates.shape, F32),
            jax.ShapeDtypeStruct((queries_here, TOPN), F32),
        ),
        in_specs=[
            vmem,
            pl.BlockSpec(memory_space=pl.ANY),
            pl.BlockSpec(memory_space=pltpu.SMEM),
            vmem,
            vmem,
        ],
        out_specs=(vmem, vmem),
        scratch_shapes=[
            pltpu.VMEM((width, cols), BF16),
            pltpu.VMEM((n, width, cols), BF16),
            pltpu.VMEM((count // 2, span, 2 * width), BF16),
            pltpu.VMEM((2 * width, 2 * cols), BF16),
            pltpu.VMEM((count // 2, 2 * cols), F32),
            pltpu.VMEM((n, 2, cols), F32),
            pltpu.VMEM((n, 2, cols), F32),
            pltpu.SemaphoreType.DMA((2,)),
            pltpu.SemaphoreType.DMA((n,)),
            pltpu.SemaphoreType.DMA((n,)),
            pltpu.SemaphoreType.DMA((n,)),
            pltpu.SemaphoreType.DMA((n,)),
            pltpu.SemaphoreType.DMA((n,)),
            pltpu.SemaphoreType.REGULAR((n,)),
        ],
        compiler_params=pltpu.CompilerParams(collective_id=0, has_side_effects=True),
    )(queries, passages, lengths, slot_of.reshape(-1, 128), candidates)


def solution(mesh):
    return jax.shard_map(
        functools.partial(shards, mesh.shape["blk"]),
        mesh=mesh,
        in_specs=(
            P(("parts", "blk", "sub", "rep"), None, None),
            P(("parts", "blk"), None, None),
            P(("parts", "blk")),
            P("parts"),
            P(("parts", "blk", "sub", "rep"), None),
        ),
        out_specs=(
            P(("parts", "blk", "sub", "rep"), None),
            P(("parts", "blk", "sub", "rep"), None),
        ),
        check_vma=False,
    )
```

```python
import functools

import jax
import jax.numpy as jnp
from jax import lax
from jax.experimental import pallas as pl
from jax.experimental.pallas import tpu as pltpu
from jax.sharding import PartitionSpec as P

MESH = pl.DeviceIdType.MESH
TOPN = 10
REACH = 4
LAG = 15
ORDER = [
    [1, 2, 3, 4, 5, 15, 6, 7, 11, 9, 8, 13, 12, 10, 14],
    [3, 7, 9, 8, 6, 4, 5, 10, 12, 11, 13, 0, 14, 15, 2],
    [1, 4, 7, 6, 9, 8, 3, 10, 5, 0, 11, 12, 13, 14, 15],
    [1, 2, 9, 6, 8, 0, 5, 4, 10, 11, 13, 12, 14, 7, 15],
    [1, 2, 3, 0, 8, 9, 5, 7, 10, 11, 6, 12, 13, 14, 15],
    [1, 2, 3, 4, 7, 0, 8, 6, 9, 10, 11, 12, 13, 14, 15],
    [1, 2, 3, 4, 5, 0, 9, 8, 10, 7, 11, 12, 13, 14, 15],
    [1, 2, 3, 4, 5, 8, 6, 0, 9, 10, 11, 13, 14, 15, 12],
    [1, 2, 3, 5, 4, 9, 6, 7, 0, 11, 10, 12, 13, 14, 15],
    [1, 2, 3, 8, 5, 4, 6, 7, 0, 13, 11, 10, 12, 14, 15],
    [1, 2, 3, 4, 5, 12, 6, 7, 11, 0, 8, 9, 13, 14, 15],
    [1, 2, 3, 13, 4, 5, 0, 6, 7, 12, 10, 8, 9, 14, 15],
    [1, 2, 3, 4, 5, 0, 6, 7, 10, 8, 9, 11, 14, 13, 15],
    [1, 2, 3, 0, 4, 14, 5, 6, 7, 12, 8, 9, 11, 15, 10],
    [1, 2, 0, 3, 4, 5, 6, 7, 12, 8, 9, 11, 13, 10, 15],
    [0, 1, 2, 3, 4, 5, 6, 7, 8, 9, 11, 10, 12, 13, 14],
]
F32 = jnp.float32
BF16 = jnp.bfloat16


def picked_by(table, me):
    words = []
    for start in range(0, len(table[0]), 5):
        word = jnp.int32(0)
        for z, line in enumerate(table):
            packed = sum(value * 32**i for i, value in enumerate(line[start : start + 5]))
            word = jnp.where(me == z, packed, word)
        words.append(word)

    def pick(at):
        word = words[-1]
        for i in range(len(words) - 1):
            word = jnp.where(at // 5 == i, words[i], word)
        return lax.rem(lax.shift_right_logical(word, 5 * lax.rem(at, 5)), 32)

    return pick


def gather_rows(table, row_of, lane_of):
    found = jnp.zeros(row_of.shape, table.dtype)
    for row in range(table.shape[0]):
        line = jnp.broadcast_to(table[row : row + 1, :], row_of.shape)
        picked = jnp.take_along_axis(line, lane_of, axis=1, mode="promise_in_bounds")
        found = jnp.where(row_of == row, picked, found)
    return found


def kernel(
    n, q_ref, p_hbm, len_ref, slot_ref, cand_ref, score_ref, top_ref,
    own, held, stored, weights, best, outgoing, table, load_sem, up_send, down_send, recv_sem, back_send, back_recv, here,
):
    me = lax.axis_index("blk")
    count, span, width = p_hbm.shape
    pairs = count // 2
    queries_here, tokens = q_ref.shape[0], q_ref.shape[1]
    cols = queries_here * tokens

    last = n - 1

    loads = []
    for side in range(2):
        load = pltpu.make_async_copy(
            p_hbm.at[pl.ds(side * pairs, pairs)],
            stored.at[:, :, pl.ds(side * width, width)],
            load_sem.at[side],
        )
        load.start()
        loads.append(load)

    flat = q_ref[...].reshape(cols, width).astype(F32)
    own[...] = flat.T.astype(BF16)
    weights[...] = jnp.zeros_like(weights)

    def climb(k, src):
        return pltpu.make_async_remote_copy(
            src_ref=src, dst_ref=held.at[k], send_sem=up_send.at[k], recv_sem=recv_sem.at[k],
            device_id={"blk": lax.rem(me + 1, n)}, device_id_type=MESH,
        )

    def direct(k):
        return pltpu.make_async_remote_copy(
            src_ref=own, dst_ref=held.at[me], send_sem=down_send.at[k], recv_sem=recv_sem.at[me],
            device_id={"blk": k}, device_id_type=MESH,
        )

    def back(k):
        return pltpu.make_async_remote_copy(
            src_ref=outgoing.at[k], dst_ref=table.at[me], send_sem=back_send.at[k], recv_sem=back_recv.at[me],
            device_id={"blk": k}, device_id_type=MESH,
        )

    def loop(low, high, step):
        def one(k, _):
            step(k)
            return 0

        lax.fori_loop(low, high, one, 0)

    barrier = pltpu.get_barrier_semaphore()

    @pl.when(me > 1)
    def _():
        pl.semaphore_wait(barrier, 1)

    @pl.when(me > 0)
    def _():
        pl.semaphore_signal(barrier, inc=1, device_id={"blk": 0}, device_id_type=MESH)

    @pl.when((me > 0) & (me < last))
    def _():
        pl.semaphore_signal(barrier, inc=1, device_id={"blk": lax.rem(me + 1, n)}, device_id_type=MESH)

    @pl.when(me > 1)
    def _():
        pl.semaphore_signal(here, inc=1, device_id={"blk": lax.rem(me + last, n)}, device_id_type=MESH)

    near = jnp.maximum(1, me - REACH)

    @pl.when(me > 0)
    def _():
        @pl.when(me - 1 > REACH)
        def _():
            direct(jnp.int32(1)).start()

        loop(near, me, lambda k: direct(k).start())

    cand = jnp.concatenate(
        [cand_ref[q : q + 1, h * 128 : (h + 1) * 128] for q in range(queries_here) for h in range(2)], axis=0
    )
    rows = gather_rows(slot_ref[...], cand // 128, cand % 128)
    query_of = lax.broadcasted_iota(jnp.int32, rows.shape, 0) // 2

    for load in loads:
        load.wait()

    def keep_live(pair, _):
        for side in range(2):
            lanes = pl.ds(side * width, width)
            piece = stored[pair, :, lanes].astype(F32)
            live = lax.broadcasted_iota(jnp.int32, piece.shape, 0) < len_ref[pair + side * pairs]
            stored[pair, :, lanes] = jnp.where(live, piece, piece[0:1, :]).astype(BF16)
        return 0

    lax.fori_loop(0, pairs, keep_live, 0)

    r_at = lax.broadcasted_iota(jnp.int32, (2 * cols, cols), 0) % cols
    c_at = lax.broadcasted_iota(jnp.int32, (2 * cols, cols), 1)
    ones_of = jnp.where(r_at // tokens == c_at // tokens, 1.0 / tokens, 0.0).astype(BF16)
    mine = (
        lax.broadcasted_iota(jnp.int32, (pairs, cols), 0) == lax.broadcasted_iota(jnp.int32, (pairs, cols), 1) % tokens
    )

    def score_block(query_cols):
        weights[0:width, 0:cols] = query_cols
        weights[width : 2 * width, cols : 2 * cols] = query_cols
        rhs = weights[...]
        for pair in range(pairs):
            similar = jnp.dot(stored[pair], rhs, preferred_element_type=F32)
            best[pair : pair + 1, :] = jnp.max(similar, axis=0, keepdims=True)
        lines = []
        for side in range(2):
            value = best[:, side * cols : (side + 1) * cols]
            high = value.astype(BF16)
            low = (value - high.astype(F32)).astype(BF16)
            summed = jnp.dot(jnp.concatenate([high, low], axis=1), ones_of, preferred_element_type=F32)
            lines.append(jnp.sum(jnp.where(mine, summed, 0.0), axis=0, keepdims=True))
        return jnp.concatenate(lines, axis=0)

    def arrived(k):
        pltpu.make_async_remote_copy(
            src_ref=own, dst_ref=held.at[k], send_sem=up_send.at[k], recv_sem=recv_sem.at[k],
            device_id={"blk": me}, device_id_type=MESH,
        ).wait_recv()

    def landed(k):
        pltpu.make_async_remote_copy(
            src_ref=outgoing.at[k], dst_ref=table.at[k], send_sem=back_send.at[k], recv_sem=back_recv.at[k],
            device_id={"blk": me}, device_id_type=MESH,
        ).wait_recv()

    table[me] = score_block(own[...])

    source_at = picked_by(ORDER, me)

    def answer(k):
        outgoing[k] = score_block(held[k])
        back(k).start()

    @pl.when(me == 0)
    def _():
        def step(t):
            @pl.when(t < last)
            def _():
                pl.semaphore_wait(barrier, 1)
                direct(t + 1).start()

            @pl.when(t >= LAG)
            def _():
                k = source_at(jnp.maximum(t - LAG, 0))
                arrived(k)
                answer(k)

        loop(0, last + LAG, step)

    @pl.when(me == 1)
    def _():
        pl.semaphore_wait(here, 1)
        climb(me, own).start()

    @pl.when(me > 0)
    def _():
        def step(t):
            k = source_at(t)
            arrived(k)

            @pl.when(k == 0)
            def _():
                direct(k).start()

            @pl.when((t == 0) & (me > 1) & (me < last))
            def _():
                pl.semaphore_wait(here, 1)

            @pl.when(((k > 0) & (k < me) & (me < last)) | (k - me > REACH + 1))
            def _():
                climb(k, held.at[k]).start()

            @pl.when((t == 0) & (me > 1) & (me < last))
            def _():
                climb(me, own).start()

            answer(k)

        loop(0, last, step)

    loop(0, me, landed)
    loop(me + 1, n, landed)

    lines = table[...].reshape(2 * n, cols)
    score = gather_rows(lines, rows // tokens, query_of * tokens + rows % tokens)
    for q in range(queries_here):
        for h in range(2):
            score_ref[q : q + 1, h * 128 : (h + 1) * 128] = score[2 * q + h : 2 * q + h + 1, :]

    down = score.T
    j_at = lax.broadcasted_iota(jnp.int32, (128, 128), 0)
    k_at = lax.broadcasted_iota(jnp.int32, (128, 128), 1)
    place = lax.broadcasted_iota(jnp.int32, (16, 128), 0).astype(F32)
    spot = lax.broadcasted_iota(jnp.int32, (16, 128), 0) == lax.broadcasted_iota(jnp.int32, (16, 128), 1)
    for q in range(queries_here):
        total = jnp.zeros((16, 1), F32)
        for kh in range(2):
            k_val = score[2 * q + kh : 2 * q + kh + 1, :]
            rank = jnp.zeros((1, 128), F32)
            for jh in range(2):
                j_val = down[:, 2 * q + jh : 2 * q + jh + 1]
                if jh < kh:
                    ahead = j_val >= k_val
                elif jh > kh:
                    ahead = j_val > k_val
                else:
                    ahead = (j_val > k_val) | ((j_val == k_val) & (j_at < k_at))
                rank = rank + jnp.sum(jnp.where(ahead, 1.0, 0.0), axis=0, keepdims=True)
            total = total + jnp.sum(jnp.where(rank == place, k_val, 0.0), axis=1, keepdims=True)
        line = jnp.sum(jnp.where(spot, total, 0.0), axis=0, keepdims=True)
        top_ref[q : q + 1, :] = line[:, 0:TOPN]

    @pl.when((me > 0) & (me < last))
    def _():
        loop(1, me, lambda k: climb(k, held.at[k]).wait_send())
        climb(me, own).wait_send()
        loop(me + REACH + 2, n, lambda k: climb(k, held.at[k]).wait_send())

    @pl.when(me == 0)
    def _():
        loop(1, n, lambda k: direct(k).wait_send())

    @pl.when(me > 0)
    def _():
        direct(jnp.int32(0)).wait_send()

        @pl.when(me - 1 > REACH)
        def _():
            direct(jnp.int32(1)).wait_send()

        loop(near, me, lambda k: direct(k).wait_send())

    loop(0, me, lambda k: back(k).wait_send())
    loop(me + 1, n, lambda k: back(k).wait_send())


def shards(n, queries, passages, lengths, slot_of, candidates):
    queries_here, tokens, width = queries.shape
    count, span, _ = passages.shape
    cols = queries_here * tokens
    vmem = pl.BlockSpec(memory_space=pltpu.VMEM)
    return pl.pallas_call(
        functools.partial(kernel, n),
        out_shape=(
            jax.ShapeDtypeStruct(candidates.shape, F32),
            jax.ShapeDtypeStruct((queries_here, TOPN), F32),
        ),
        in_specs=[
            vmem,
            pl.BlockSpec(memory_space=pl.ANY),
            pl.BlockSpec(memory_space=pltpu.SMEM),
            vmem,
            vmem,
        ],
        out_specs=(vmem, vmem),
        scratch_shapes=[
            pltpu.VMEM((width, cols), BF16),
            pltpu.VMEM((n, width, cols), BF16),
            pltpu.VMEM((count // 2, span, 2 * width), BF16),
            pltpu.VMEM((2 * width, 2 * cols), BF16),
            pltpu.VMEM((count // 2, 2 * cols), F32),
            pltpu.VMEM((n, 2, cols), F32),
            pltpu.VMEM((n, 2, cols), F32),
            pltpu.SemaphoreType.DMA((2,)),
            pltpu.SemaphoreType.DMA((n,)),
            pltpu.SemaphoreType.DMA((n,)),
            pltpu.SemaphoreType.DMA((n,)),
            pltpu.SemaphoreType.DMA((n,)),
            pltpu.SemaphoreType.DMA((n,)),
            pltpu.SemaphoreType.REGULAR,
        ],
        compiler_params=pltpu.CompilerParams(collective_id=0, has_side_effects=True),
    )(queries, passages, lengths, slot_of.reshape(-1, 128), candidates)


def solution(mesh):
    return jax.shard_map(
        functools.partial(shards, mesh.shape["blk"]),
        mesh=mesh,
        in_specs=(
            P(("parts", "blk", "sub", "rep"), None, None),
            P(("parts", "blk"), None, None),
            P(("parts", "blk")),
            P("parts"),
            P(("parts", "blk", "sub", "rep"), None),
        ),
        out_specs=(
            P(("parts", "blk", "sub", "rep"), None),
            P(("parts", "blk", "sub", "rep"), None),
        ),
        check_vma=False,
    )
```

```python
import functools

import jax
import jax.numpy as jnp
from jax import lax
from jax.experimental import pallas as pl
from jax.experimental.pallas import tpu as pltpu
from jax.sharding import PartitionSpec as P

MESH = pl.DeviceIdType.MESH
TOPN = 10
REACH = 6
LAG = 13
ORDER = [
    [9, 1, 4, 13, 10, 5, 2, 3, 11, 15, 8, 6, 7, 14, 12],
    [5, 6, 9, 7, 2, 8, 10, 3, 4, 12, 11, 13, 0, 14, 15],
    [1, 5, 10, 9, 3, 11, 13, 7, 12, 6, 14, 15, 0, 4, 8],
    [1, 2, 7, 10, 5, 4, 0, 8, 6, 11, 13, 12, 14, 15, 9],
    [1, 2, 3, 5, 10, 9, 0, 8, 11, 12, 13, 7, 14, 15, 6],
    [1, 2, 3, 4, 9, 6, 0, 8, 7, 12, 13, 10, 14, 15, 11],
    [1, 2, 3, 4, 5, 9, 10, 7, 0, 11, 12, 14, 15, 8, 13],
    [1, 2, 3, 4, 5, 6, 0, 8, 13, 11, 12, 10, 9, 14, 15],
    [1, 2, 3, 4, 5, 7, 6, 10, 0, 9, 11, 13, 12, 14, 15],
    [1, 2, 3, 4, 5, 6, 7, 8, 0, 10, 15, 11, 12, 14, 13],
    [1, 2, 3, 4, 5, 6, 7, 8, 9, 14, 0, 15, 13, 12, 11],
    [1, 2, 3, 4, 5, 6, 7, 8, 9, 10, 0, 12, 14, 13, 15],
    [1, 2, 3, 4, 5, 0, 6, 7, 8, 9, 10, 11, 14, 15, 13],
    [1, 0, 2, 3, 4, 5, 6, 7, 8, 9, 10, 11, 12, 14, 15],
    [0, 1, 2, 3, 4, 5, 6, 7, 8, 9, 10, 11, 15, 12, 13],
    [0, 1, 2, 3, 4, 5, 6, 7, 8, 9, 10, 11, 12, 13, 14],
]
F32 = jnp.float32
BF16 = jnp.bfloat16


def picked_by(table, me):
    words = []
    for start in range(0, len(table[0]), 5):
        word = jnp.int32(0)
        for z, line in enumerate(table):
            packed = sum(value * 32**i for i, value in enumerate(line[start : start + 5]))
            word = jnp.where(me == z, packed, word)
        words.append(word)

    def pick(at):
        word = words[-1]
        for i in range(len(words) - 1):
            word = jnp.where(at // 5 == i, words[i], word)
        return lax.rem(lax.shift_right_logical(word, 5 * lax.rem(at, 5)), 32)

    return pick


def gather_rows(table, row_of, lane_of):
    found = jnp.zeros(row_of.shape, table.dtype)
    for row in range(table.shape[0]):
        line = jnp.broadcast_to(table[row : row + 1, :], row_of.shape)
        picked = jnp.take_along_axis(line, lane_of, axis=1, mode="promise_in_bounds")
        found = jnp.where(row_of == row, picked, found)
    return found


def kernel(
    n, q_ref, p_hbm, len_ref, table,
    own, held, stored, weights, best, outgoing, load_sem, up_send, down_send, recv_sem, back_send, back_recv, here,
):
    me = lax.axis_index("blk")
    count, span, width = p_hbm.shape
    pairs = count // 2
    queries_here, tokens = q_ref.shape[0], q_ref.shape[1]
    cols = queries_here * tokens

    last = n - 1

    loads = []
    for side in range(2):
        load = pltpu.make_async_copy(
            p_hbm.at[pl.ds(side * pairs, pairs)],
            stored.at[:, :, pl.ds(side * width, width)],
            load_sem.at[side],
        )
        load.start()
        loads.append(load)

    flat = q_ref[...].reshape(cols, width).astype(F32)
    own[...] = flat.T.astype(BF16)
    weights[...] = jnp.zeros_like(weights)

    def climb(k, src):
        return pltpu.make_async_remote_copy(
            src_ref=src, dst_ref=held.at[k], send_sem=up_send.at[k], recv_sem=recv_sem.at[k],
            device_id={"blk": lax.rem(me + 1, n)}, device_id_type=MESH,
        )

    def direct(k):
        return pltpu.make_async_remote_copy(
            src_ref=own, dst_ref=held.at[me], send_sem=down_send.at[k], recv_sem=recv_sem.at[me],
            device_id={"blk": k}, device_id_type=MESH,
        )

    def to_bottom(k):
        return pltpu.make_async_remote_copy(
            src_ref=held.at[k], dst_ref=held.at[k], send_sem=down_send.at[k], recv_sem=recv_sem.at[k],
            device_id={"blk": 0}, device_id_type=MESH,
        )

    def back(k):
        return pltpu.make_async_remote_copy(
            src_ref=outgoing.at[k], dst_ref=table.at[me], send_sem=back_send.at[k], recv_sem=back_recv.at[me],
            device_id={"blk": k}, device_id_type=MESH,
        )

    def loop(low, high, step):
        def one(k, _):
            step(k)
            return 0

        lax.fori_loop(low, high, one, 0)

    barrier = pltpu.get_barrier_semaphore()

    @pl.when(me > 1)
    def _():
        pl.semaphore_wait(barrier, 1)

    @pl.when(me > 0)
    def _():
        pl.semaphore_signal(barrier, inc=1, device_id={"blk": 0}, device_id_type=MESH)

    @pl.when((me > 0) & (me < last))
    def _():
        pl.semaphore_signal(barrier, inc=1, device_id={"blk": lax.rem(me + 1, n)}, device_id_type=MESH)

    @pl.when(me > 1)
    def _():
        pl.semaphore_signal(here, inc=1, device_id={"blk": lax.rem(me + last, n)}, device_id_type=MESH)

    near = jnp.maximum(1, me - REACH)

    @pl.when(me > 0)
    def _():
        @pl.when(me - 1 > REACH)
        def _():
            direct(jnp.int32(1)).start()

        loop(near, me, lambda k: direct(k).start())

    for load in loads:
        load.wait()

    def keep_live(pair, _):
        for side in range(2):
            lanes = pl.ds(side * width, width)
            piece = stored[pair, :, lanes].astype(F32)
            live = lax.broadcasted_iota(jnp.int32, piece.shape, 0) < len_ref[pair + side * pairs]
            stored[pair, :, lanes] = jnp.where(live, piece, piece[0:1, :]).astype(BF16)
        return 0

    lax.fori_loop(0, pairs, keep_live, 0)

    r_at = lax.broadcasted_iota(jnp.int32, (2 * cols, cols), 0) % cols
    c_at = lax.broadcasted_iota(jnp.int32, (2 * cols, cols), 1)
    ones_of = jnp.where(r_at // tokens == c_at // tokens, 1.0 / tokens, 0.0).astype(BF16)
    mine = (
        lax.broadcasted_iota(jnp.int32, (pairs, cols), 0) == lax.broadcasted_iota(jnp.int32, (pairs, cols), 1) % tokens
    )

    def score_block(query_cols):
        weights[0:width, 0:cols] = query_cols
        weights[width : 2 * width, cols : 2 * cols] = query_cols
        rhs = weights[...]
        for pair in range(pairs):
            similar = jnp.dot(stored[pair], rhs, preferred_element_type=F32)
            best[pair : pair + 1, :] = jnp.max(similar, axis=0, keepdims=True)
        lines = []
        for side in range(2):
            value = best[:, side * cols : (side + 1) * cols]
            high = value.astype(BF16)
            low = (value - high.astype(F32)).astype(BF16)
            summed = jnp.dot(jnp.concatenate([high, low], axis=1), ones_of, preferred_element_type=F32)
            lines.append(jnp.sum(jnp.where(mine, summed, 0.0), axis=0, keepdims=True))
        return jnp.concatenate(lines, axis=0)

    def arrived(k):
        pltpu.make_async_remote_copy(
            src_ref=own, dst_ref=held.at[k], send_sem=up_send.at[k], recv_sem=recv_sem.at[k],
            device_id={"blk": me}, device_id_type=MESH,
        ).wait_recv()

    def landed(k):
        pltpu.make_async_remote_copy(
            src_ref=outgoing.at[k], dst_ref=table.at[k], send_sem=back_send.at[k], recv_sem=back_recv.at[k],
            device_id={"blk": me}, device_id_type=MESH,
        ).wait_recv()

    table[me] = score_block(own[...])

    source_at = picked_by(ORDER, me)
    met = ORDER[1].index(0)

    def answer(k):
        outgoing[k] = score_block(held[k])
        back(k).start()

    @pl.when(me == 0)
    def _():
        def step(t):
            @pl.when(t < last)
            def _():
                pl.semaphore_wait(barrier, 1)
                direct(t + 1).start()

            @pl.when(t >= LAG)
            def _():
                k = source_at(jnp.maximum(t - LAG, 0))
                arrived(k)
                answer(k)

        loop(0, last + LAG, step)

    @pl.when(me == 1)
    def _():
        pl.semaphore_wait(here, 1)
        climb(me, own).start()

    @pl.when(me > 0)
    def _():
        def step(t):
            k = source_at(t)
            arrived(k)

            @pl.when((k == 0) & (me - 1 <= REACH))
            def _():
                direct(k).start()

            @pl.when((k == 0) & (me == 1))
            def _():
                for far in ORDER[1][:met]:
                    if far - 1 > REACH:
                        to_bottom(jnp.int32(far)).start()

            @pl.when((t > met) & (me == 1) & (k - 1 > REACH))
            def _():
                to_bottom(k).start()

            @pl.when((t == 0) & (me > 1) & (me < last))
            def _():
                pl.semaphore_wait(here, 1)

            @pl.when(((k > 0) & (k < me) & (me < last)) | (k - me > REACH + 1))
            def _():
                climb(k, held.at[k]).start()

            @pl.when((t == 0) & (me > 1) & (me < last))
            def _():
                climb(me, own).start()

            answer(k)

        loop(0, last, step)

    loop(0, me, landed)
    loop(me + 1, n, landed)

    @pl.when((me > 0) & (me < last))
    def _():
        loop(1, me, lambda k: climb(k, held.at[k]).wait_send())
        climb(me, own).wait_send()
        loop(me + REACH + 2, n, lambda k: climb(k, held.at[k]).wait_send())

    @pl.when(me == 0)
    def _():
        loop(1, n, lambda k: direct(k).wait_send())

    @pl.when(me == 1)
    def _():
        loop(REACH + 2, n, lambda k: to_bottom(k).wait_send())

    @pl.when(me > 0)
    def _():
        direct(jnp.where(me - 1 > REACH, 1, 0)).wait_send()

        loop(near, me, lambda k: direct(k).wait_send())

    loop(0, me, lambda k: back(k).wait_send())
    loop(me + 1, n, lambda k: back(k).wait_send())


def finish(slot_ref, cand_ref, table, score_ref, top_ref):
    n, _, cols = table.shape
    queries_here = cand_ref.shape[0]
    tokens = cols // queries_here
    cand = jnp.concatenate(
        [cand_ref[q : q + 1, h * 128 : (h + 1) * 128] for q in range(queries_here) for h in range(2)], axis=0
    )
    rows = gather_rows(slot_ref[...], cand // 128, cand % 128)
    query_of = lax.broadcasted_iota(jnp.int32, rows.shape, 0) // 2

    lines = table[...].reshape(2 * n, cols)
    score = gather_rows(lines, rows // tokens, query_of * tokens + rows % tokens)
    for q in range(queries_here):
        for h in range(2):
            score_ref[q : q + 1, h * 128 : (h + 1) * 128] = score[2 * q + h : 2 * q + h + 1, :]

    down = score.T
    j_at = lax.broadcasted_iota(jnp.int32, (128, 128), 0)
    k_at = lax.broadcasted_iota(jnp.int32, (128, 128), 1)
    place = lax.broadcasted_iota(jnp.int32, (16, 128), 0).astype(F32)
    spot = lax.broadcasted_iota(jnp.int32, (16, 128), 0) == lax.broadcasted_iota(jnp.int32, (16, 128), 1)
    for q in range(queries_here):
        total = jnp.zeros((16, 1), F32)
        for kh in range(2):
            k_val = score[2 * q + kh : 2 * q + kh + 1, :]
            rank = jnp.zeros((1, 128), F32)
            for jh in range(2):
                j_val = down[:, 2 * q + jh : 2 * q + jh + 1]
                if jh < kh:
                    ahead = j_val >= k_val
                elif jh > kh:
                    ahead = j_val > k_val
                else:
                    ahead = (j_val > k_val) | ((j_val == k_val) & (j_at < k_at))
                rank = rank + jnp.sum(jnp.where(ahead, 1.0, 0.0), axis=0, keepdims=True)
            total = total + jnp.sum(jnp.where(rank == place, k_val, 0.0), axis=1, keepdims=True)
        line = jnp.sum(jnp.where(spot, total, 0.0), axis=0, keepdims=True)
        top_ref[q : q + 1, :] = line[:, 0:TOPN]


def shards(n, queries, passages, lengths, slot_of, candidates):
    queries_here, tokens, width = queries.shape
    count, span, _ = passages.shape
    cols = queries_here * tokens
    vmem = pl.BlockSpec(memory_space=pltpu.VMEM)
    scores = pl.pallas_call(
        functools.partial(kernel, n),
        out_shape=jax.ShapeDtypeStruct((n, 2, cols), F32),
        in_specs=[vmem, pl.BlockSpec(memory_space=pl.ANY), pl.BlockSpec(memory_space=pltpu.SMEM)],
        out_specs=vmem,
        scratch_shapes=[
            pltpu.VMEM((width, cols), BF16),
            pltpu.VMEM((n, width, cols), BF16),
            pltpu.VMEM((count // 2, span, 2 * width), BF16),
            pltpu.VMEM((2 * width, 2 * cols), BF16),
            pltpu.VMEM((count // 2, 2 * cols), F32),
            pltpu.VMEM((n, 2, cols), F32),
            pltpu.SemaphoreType.DMA((2,)),
            pltpu.SemaphoreType.DMA((n,)),
            pltpu.SemaphoreType.DMA((n,)),
            pltpu.SemaphoreType.DMA((n,)),
            pltpu.SemaphoreType.DMA((n,)),
            pltpu.SemaphoreType.DMA((n,)),
            pltpu.SemaphoreType.REGULAR,
        ],
        compiler_params=pltpu.CompilerParams(collective_id=0, has_side_effects=True),
    )(queries, passages, lengths)
    return pl.pallas_call(
        finish,
        out_shape=(
            jax.ShapeDtypeStruct(candidates.shape, F32),
            jax.ShapeDtypeStruct((queries_here, TOPN), F32),
        ),
        in_specs=[vmem] * 3,
        out_specs=(vmem, vmem),
    )(slot_of.reshape(-1, 128), candidates, scores)


def solution(mesh):
    return jax.shard_map(
        functools.partial(shards, mesh.shape["blk"]),
        mesh=mesh,
        in_specs=(
            P(("parts", "blk", "sub", "rep"), None, None),
            P(("parts", "blk"), None, None),
            P(("parts", "blk")),
            P("parts"),
            P(("parts", "blk", "sub", "rep"), None),
        ),
        out_specs=(
            P(("parts", "blk", "sub", "rep"), None),
            P(("parts", "blk", "sub", "rep"), None),
        ),
        check_vma=False,
    )
```

```python
import functools

import jax
import jax.numpy as jnp
from jax import lax
from jax.experimental import pallas as pl
from jax.experimental.pallas import tpu as pltpu
from jax.sharding import PartitionSpec as P

MESH = pl.DeviceIdType.MESH
TOPN = 10
REACH = 4
LAG = 15
ORDER = [
    [1, 2, 3, 4, 5, 15, 6, 7, 11, 9, 8, 13, 12, 10, 14],
    [3, 7, 9, 8, 6, 4, 5, 10, 12, 11, 13, 0, 14, 15, 2],
    [1, 4, 7, 6, 9, 8, 3, 10, 5, 0, 11, 12, 13, 14, 15],
    [1, 2, 9, 6, 8, 0, 5, 4, 10, 11, 13, 12, 14, 7, 15],
    [1, 2, 3, 0, 8, 9, 5, 7, 10, 11, 6, 12, 13, 14, 15],
    [1, 2, 3, 4, 7, 0, 8, 6, 9, 10, 11, 12, 13, 14, 15],
    [1, 2, 3, 4, 5, 0, 9, 8, 10, 7, 11, 12, 13, 14, 15],
    [1, 2, 3, 4, 5, 8, 6, 0, 9, 10, 11, 13, 14, 15, 12],
    [1, 2, 3, 5, 4, 9, 6, 7, 0, 11, 10, 12, 13, 14, 15],
    [1, 2, 3, 8, 5, 4, 6, 7, 0, 13, 11, 10, 12, 14, 15],
    [1, 2, 3, 4, 5, 12, 6, 7, 11, 0, 8, 9, 13, 14, 15],
    [1, 2, 3, 13, 4, 5, 0, 6, 7, 12, 10, 8, 9, 14, 15],
    [1, 2, 3, 4, 5, 0, 6, 7, 10, 8, 9, 11, 14, 13, 15],
    [1, 2, 3, 0, 4, 14, 5, 6, 7, 12, 8, 9, 11, 15, 10],
    [1, 2, 0, 3, 4, 5, 6, 7, 12, 8, 9, 11, 13, 10, 15],
    [0, 1, 2, 3, 4, 5, 6, 7, 8, 9, 11, 10, 12, 13, 14],
]
F32 = jnp.float32
BF16 = jnp.bfloat16


def picked_by(table, me):
    words = []
    for start in range(0, len(table[0]), 5):
        word = jnp.int32(0)
        for z, line in enumerate(table):
            packed = sum(value * 32**i for i, value in enumerate(line[start : start + 5]))
            word = jnp.where(me == z, packed, word)
        words.append(word)

    def pick(at):
        word = words[-1]
        for i in range(len(words) - 1):
            word = jnp.where(at // 5 == i, words[i], word)
        return lax.rem(lax.shift_right_logical(word, 5 * lax.rem(at, 5)), 32)

    return pick


def gather_rows(table, row_of, lane_of):
    found = jnp.zeros(row_of.shape, table.dtype)
    for row in range(table.shape[0]):
        line = jnp.broadcast_to(table[row : row + 1, :], row_of.shape)
        picked = jnp.take_along_axis(line, lane_of, axis=1, mode="promise_in_bounds")
        found = jnp.where(row_of == row, picked, found)
    return found


def kernel(
    n, q_ref, p_hbm, len_ref, table,
    own, held, stored, weights, best, outgoing, load_sem, up_send, down_send, recv_sem, back_send, back_recv, here,
):
    me = lax.axis_index("blk")
    count, span, width = p_hbm.shape
    pairs = count // 2
    queries_here, tokens = q_ref.shape[0], q_ref.shape[1]
    cols = queries_here * tokens

    last = n - 1

    loads = []
    for side in range(2):
        load = pltpu.make_async_copy(
            p_hbm.at[pl.ds(side * pairs, pairs)],
            stored.at[:, :, pl.ds(side * width, width)],
            load_sem.at[side],
        )
        load.start()
        loads.append(load)

    flat = q_ref[...].reshape(cols, width).astype(F32)
    own[...] = flat.T.astype(BF16)
    weights[...] = jnp.zeros_like(weights)

    def climb(k, src):
        return pltpu.make_async_remote_copy(
            src_ref=src, dst_ref=held.at[k], send_sem=up_send.at[k], recv_sem=recv_sem.at[k],
            device_id={"blk": lax.rem(me + 1, n)}, device_id_type=MESH,
        )

    def direct(k):
        return pltpu.make_async_remote_copy(
            src_ref=own, dst_ref=held.at[me], send_sem=down_send.at[k], recv_sem=recv_sem.at[me],
            device_id={"blk": k}, device_id_type=MESH,
        )

    def back(k):
        return pltpu.make_async_remote_copy(
            src_ref=outgoing.at[k], dst_ref=table.at[me], send_sem=back_send.at[k], recv_sem=back_recv.at[me],
            device_id={"blk": k}, device_id_type=MESH,
        )

    def loop(low, high, step):
        def one(k, _):
            step(k)
            return 0

        lax.fori_loop(low, high, one, 0)

    barrier = pltpu.get_barrier_semaphore()

    @pl.when(me > 1)
    def _():
        pl.semaphore_wait(barrier, 1)

    @pl.when(me > 0)
    def _():
        pl.semaphore_signal(barrier, inc=1, device_id={"blk": 0}, device_id_type=MESH)

    @pl.when((me > 0) & (me < last))
    def _():
        pl.semaphore_signal(barrier, inc=1, device_id={"blk": lax.rem(me + 1, n)}, device_id_type=MESH)

    @pl.when(me > 1)
    def _():
        pl.semaphore_signal(here, inc=1, device_id={"blk": lax.rem(me + last, n)}, device_id_type=MESH)

    near = jnp.maximum(1, me - REACH)

    @pl.when(me > 0)
    def _():
        @pl.when(me - 1 > REACH)
        def _():
            direct(jnp.int32(1)).start()

        loop(near, me, lambda k: direct(k).start())

    for load in loads:
        load.wait()

    def keep_live(pair, _):
        for side in range(2):
            lanes = pl.ds(side * width, width)
            piece = stored[pair, :, lanes].astype(F32)
            live = lax.broadcasted_iota(jnp.int32, piece.shape, 0) < len_ref[pair + side * pairs]
            stored[pair, :, lanes] = jnp.where(live, piece, piece[0:1, :]).astype(BF16)
        return 0

    lax.fori_loop(0, pairs, keep_live, 0)

    r_at = lax.broadcasted_iota(jnp.int32, (2 * cols, cols), 0) % cols
    c_at = lax.broadcasted_iota(jnp.int32, (2 * cols, cols), 1)
    ones_of = jnp.where(r_at // tokens == c_at // tokens, 1.0 / tokens, 0.0).astype(BF16)
    mine = (
        lax.broadcasted_iota(jnp.int32, (pairs, cols), 0) == lax.broadcasted_iota(jnp.int32, (pairs, cols), 1) % tokens
    )

    def score_block(query_cols):
        weights[0:width, 0:cols] = query_cols
        weights[width : 2 * width, cols : 2 * cols] = query_cols
        rhs = weights[...]
        for pair in range(pairs):
            similar = jnp.dot(stored[pair], rhs, preferred_element_type=F32)
            best[pair : pair + 1, :] = jnp.max(similar, axis=0, keepdims=True)
        lines = []
        for side in range(2):
            value = best[:, side * cols : (side + 1) * cols]
            high = value.astype(BF16)
            low = (value - high.astype(F32)).astype(BF16)
            summed = jnp.dot(jnp.concatenate([high, low], axis=1), ones_of, preferred_element_type=F32)
            lines.append(jnp.sum(jnp.where(mine, summed, 0.0), axis=0, keepdims=True))
        return jnp.concatenate(lines, axis=0)

    def arrived(k):
        pltpu.make_async_remote_copy(
            src_ref=own, dst_ref=held.at[k], send_sem=up_send.at[k], recv_sem=recv_sem.at[k],
            device_id={"blk": me}, device_id_type=MESH,
        ).wait_recv()

    def landed(k):
        pltpu.make_async_remote_copy(
            src_ref=outgoing.at[k], dst_ref=table.at[k], send_sem=back_send.at[k], recv_sem=back_recv.at[k],
            device_id={"blk": me}, device_id_type=MESH,
        ).wait_recv()

    table[me] = score_block(own[...])

    source_at = picked_by(ORDER, me)

    def answer(k):
        outgoing[k] = score_block(held[k])
        back(k).start()

    @pl.when(me == 0)
    def _():
        def step(t):
            @pl.when(t < last)
            def _():
                pl.semaphore_wait(barrier, 1)
                direct(t + 1).start()

            @pl.when(t >= LAG)
            def _():
                k = source_at(jnp.maximum(t - LAG, 0))
                arrived(k)
                answer(k)

        loop(0, last + LAG, step)

    @pl.when(me == 1)
    def _():
        pl.semaphore_wait(here, 1)
        climb(me, own).start()

    @pl.when(me > 0)
    def _():
        def step(t):
            k = source_at(t)
            arrived(k)

            @pl.when(k == 0)
            def _():
                direct(k).start()

            @pl.when((t == 0) & (me > 1) & (me < last))
            def _():
                pl.semaphore_wait(here, 1)

            @pl.when(((k > 0) & (k < me) & (me < last)) | (k - me > REACH + 1))
            def _():
                climb(k, held.at[k]).start()

            @pl.when((t == 0) & (me > 1) & (me < last))
            def _():
                climb(me, own).start()

            answer(k)

        loop(0, last, step)

    loop(0, me, landed)
    loop(me + 1, n, landed)

    @pl.when((me > 0) & (me < last))
    def _():
        loop(1, me, lambda k: climb(k, held.at[k]).wait_send())
        climb(me, own).wait_send()
        loop(me + REACH + 2, n, lambda k: climb(k, held.at[k]).wait_send())

    @pl.when(me == 0)
    def _():
        loop(1, n, lambda k: direct(k).wait_send())

    @pl.when(me > 0)
    def _():
        direct(jnp.int32(0)).wait_send()

        @pl.when(me - 1 > REACH)
        def _():
            direct(jnp.int32(1)).wait_send()

        loop(near, me, lambda k: direct(k).wait_send())

    loop(0, me, lambda k: back(k).wait_send())
    loop(me + 1, n, lambda k: back(k).wait_send())


def finish(slot_ref, cand_ref, table, score_ref, top_ref):
    n, _, cols = table.shape
    queries_here = cand_ref.shape[0]
    tokens = cols // queries_here
    cand = jnp.concatenate(
        [cand_ref[q : q + 1, h * 128 : (h + 1) * 128] for q in range(queries_here) for h in range(2)], axis=0
    )
    rows = gather_rows(slot_ref[...], cand // 128, cand % 128)
    query_of = lax.broadcasted_iota(jnp.int32, rows.shape, 0) // 2

    lines = table[...].reshape(2 * n, cols)
    score = gather_rows(lines, rows // tokens, query_of * tokens + rows % tokens)
    for q in range(queries_here):
        for h in range(2):
            score_ref[q : q + 1, h * 128 : (h + 1) * 128] = score[2 * q + h : 2 * q + h + 1, :]

    down = score.T
    j_at = lax.broadcasted_iota(jnp.int32, (128, 128), 0)
    k_at = lax.broadcasted_iota(jnp.int32, (128, 128), 1)
    place = lax.broadcasted_iota(jnp.int32, (16, 128), 0).astype(F32)
    spot = lax.broadcasted_iota(jnp.int32, (16, 128), 0) == lax.broadcasted_iota(jnp.int32, (16, 128), 1)
    for q in range(queries_here):
        total = jnp.zeros((16, 1), F32)
        for kh in range(2):
            k_val = score[2 * q + kh : 2 * q + kh + 1, :]
            rank = jnp.zeros((1, 128), F32)
            for jh in range(2):
                j_val = down[:, 2 * q + jh : 2 * q + jh + 1]
                if jh < kh:
                    ahead = j_val >= k_val
                elif jh > kh:
                    ahead = j_val > k_val
                else:
                    ahead = (j_val > k_val) | ((j_val == k_val) & (j_at < k_at))
                rank = rank + jnp.sum(jnp.where(ahead, 1.0, 0.0), axis=0, keepdims=True)
            total = total + jnp.sum(jnp.where(rank == place, k_val, 0.0), axis=1, keepdims=True)
        line = jnp.sum(jnp.where(spot, total, 0.0), axis=0, keepdims=True)
        top_ref[q : q + 1, :] = line[:, 0:TOPN]


def shards(n, queries, passages, lengths, slot_of, candidates):
    queries_here, tokens, width = queries.shape
    count, span, _ = passages.shape
    cols = queries_here * tokens
    vmem = pl.BlockSpec(memory_space=pltpu.VMEM)
    scores = pl.pallas_call(
        functools.partial(kernel, n),
        out_shape=jax.ShapeDtypeStruct((n, 2, cols), F32),
        in_specs=[vmem, pl.BlockSpec(memory_space=pl.ANY), pl.BlockSpec(memory_space=pltpu.SMEM)],
        out_specs=vmem,
        scratch_shapes=[
            pltpu.VMEM((width, cols), BF16),
            pltpu.VMEM((n, width, cols), BF16),
            pltpu.VMEM((count // 2, span, 2 * width), BF16),
            pltpu.VMEM((2 * width, 2 * cols), BF16),
            pltpu.VMEM((count // 2, 2 * cols), F32),
            pltpu.VMEM((n, 2, cols), F32),
            pltpu.SemaphoreType.DMA((2,)),
            pltpu.SemaphoreType.DMA((n,)),
            pltpu.SemaphoreType.DMA((n,)),
            pltpu.SemaphoreType.DMA((n,)),
            pltpu.SemaphoreType.DMA((n,)),
            pltpu.SemaphoreType.DMA((n,)),
            pltpu.SemaphoreType.REGULAR,
        ],
        compiler_params=pltpu.CompilerParams(collective_id=0, has_side_effects=True),
    )(queries, passages, lengths)
    return pl.pallas_call(
        finish,
        out_shape=(
            jax.ShapeDtypeStruct(candidates.shape, F32),
            jax.ShapeDtypeStruct((queries_here, TOPN), F32),
        ),
        in_specs=[vmem] * 3,
        out_specs=(vmem, vmem),
    )(slot_of.reshape(-1, 128), candidates, scores)


def solution(mesh):
    return jax.shard_map(
        functools.partial(shards, mesh.shape["blk"]),
        mesh=mesh,
        in_specs=(
            P(("parts", "blk", "sub", "rep"), None, None),
            P(("parts", "blk"), None, None),
            P(("parts", "blk")),
            P("parts"),
            P(("parts", "blk", "sub", "rep"), None),
        ),
        out_specs=(
            P(("parts", "blk", "sub", "rep"), None),
            P(("parts", "blk", "sub", "rep"), None),
        ),
        check_vma=False,
    )
```

```python
import functools

import jax
import jax.numpy as jnp
from jax import lax
from jax.experimental import pallas as pl
from jax.experimental.pallas import tpu as pltpu
from jax.sharding import PartitionSpec as P

MESH = pl.DeviceIdType.MESH
TOPN = 10
REACH = 5
LAG = 15
ORDER = [
    [15, 4, 1, 2, 13, 6, 3, 9, 7, 14, 5, 8, 10, 12, 11],
    [3, 6, 7, 10, 4, 8, 11, 2, 9, 14, 12, 0, 13, 5, 15],
    [1, 5, 10, 9, 6, 4, 3, 7, 0, 11, 12, 13, 8, 14, 15],
    [1, 2, 6, 5, 8, 4, 0, 9, 7, 10, 11, 13, 14, 15, 12],
    [1, 2, 3, 6, 9, 0, 8, 10, 5, 7, 11, 13, 14, 15, 12],
    [1, 2, 3, 4, 7, 6, 8, 0, 10, 11, 13, 14, 15, 9, 12],
    [1, 2, 3, 5, 4, 0, 10, 8, 11, 13, 9, 14, 15, 7, 12],
    [1, 2, 3, 5, 4, 6, 12, 10, 0, 8, 13, 11, 14, 15, 9],
    [1, 2, 3, 5, 4, 7, 6, 0, 12, 10, 11, 13, 9, 14, 15],
    [1, 2, 3, 8, 5, 4, 12, 13, 11, 6, 7, 0, 10, 14, 15],
    [1, 2, 3, 12, 5, 4, 6, 7, 8, 0, 9, 13, 11, 14, 15],
    [13, 1, 2, 3, 5, 4, 10, 6, 7, 0, 8, 9, 14, 12, 15],
    [1, 2, 3, 0, 4, 5, 6, 7, 10, 8, 9, 11, 13, 15, 14],
    [14, 0, 1, 2, 3, 4, 5, 6, 7, 8, 9, 10, 11, 12, 15],
    [0, 1, 2, 3, 13, 4, 5, 6, 7, 8, 9, 10, 11, 12, 15],
    [0, 1, 2, 3, 4, 5, 6, 7, 8, 9, 10, 11, 12, 14, 13],
]
F32 = jnp.float32
BF16 = jnp.bfloat16


def picked_by(table, me):
    words = []
    for start in range(0, len(table[0]), 5):
        word = jnp.int32(0)
        for z, line in enumerate(table):
            packed = sum(value * 32**i for i, value in enumerate(line[start : start + 5]))
            word = jnp.where(me == z, packed, word)
        words.append(word)

    def pick(at):
        word = words[-1]
        for i in range(len(words) - 1):
            word = jnp.where(at // 5 == i, words[i], word)
        return lax.rem(lax.shift_right_logical(word, 5 * lax.rem(at, 5)), 32)

    return pick


def gather_rows(table, row_of, lane_of):
    found = jnp.zeros(row_of.shape, table.dtype)
    for row in range(table.shape[0]):
        line = jnp.broadcast_to(table[row : row + 1, :], row_of.shape)
        picked = jnp.take_along_axis(line, lane_of, axis=1, mode="promise_in_bounds")
        found = jnp.where(row_of == row, picked, found)
    return found


def kernel(
    n, q_ref, p_hbm, len_ref, table,
    own, held, stored, weights, best, outgoing, load_sem, up_send, down_send, recv_sem, back_send, back_recv, here,
):
    me = lax.axis_index("blk")
    count, span, width = p_hbm.shape
    pairs = count // 2
    queries_here, tokens = q_ref.shape[0], q_ref.shape[1]
    cols = queries_here * tokens

    last = n - 1

    loads = []
    for side in range(2):
        load = pltpu.make_async_copy(
            p_hbm.at[pl.ds(side * pairs, pairs)],
            stored.at[:, :, pl.ds(side * width, width)],
            load_sem.at[side],
        )
        load.start()
        loads.append(load)

    flat = q_ref[...].reshape(cols, width).astype(F32)
    own[...] = flat.T.astype(BF16)
    weights[...] = jnp.zeros_like(weights)

    def climb(k, src):
        return pltpu.make_async_remote_copy(
            src_ref=src, dst_ref=held.at[k], send_sem=up_send.at[k], recv_sem=recv_sem.at[k],
            device_id={"blk": lax.rem(me + 1, n)}, device_id_type=MESH,
        )

    def direct(k):
        return pltpu.make_async_remote_copy(
            src_ref=own, dst_ref=held.at[me], send_sem=down_send.at[k], recv_sem=recv_sem.at[me],
            device_id={"blk": k}, device_id_type=MESH,
        )

    def back(k):
        return pltpu.make_async_remote_copy(
            src_ref=outgoing.at[k], dst_ref=table.at[me], send_sem=back_send.at[k], recv_sem=back_recv.at[me],
            device_id={"blk": k}, device_id_type=MESH,
        )

    def loop(low, high, step):
        def one(k, _):
            step(k)
            return 0

        lax.fori_loop(low, high, one, 0)

    barrier = pltpu.get_barrier_semaphore()

    @pl.when(me > 1)
    def _():
        pl.semaphore_wait(barrier, 1)

    @pl.when(me > 0)
    def _():
        pl.semaphore_signal(barrier, inc=1, device_id={"blk": 0}, device_id_type=MESH)

    @pl.when((me > 0) & (me < last))
    def _():
        pl.semaphore_signal(barrier, inc=1, device_id={"blk": lax.rem(me + 1, n)}, device_id_type=MESH)

    @pl.when(me > 1)
    def _():
        pl.semaphore_signal(here, inc=1, device_id={"blk": lax.rem(me + last, n)}, device_id_type=MESH)

    near = jnp.maximum(1, me - REACH)

    @pl.when(me > 0)
    def _():
        @pl.when(me - 1 > REACH)
        def _():
            direct(jnp.int32(1)).start()

        loop(near, me, lambda k: direct(k).start())

    for load in loads:
        load.wait()

    def keep_live(pair, _):
        for side in range(2):
            lanes = pl.ds(side * width, width)
            piece = stored[pair, :, lanes].astype(F32)
            live = lax.broadcasted_iota(jnp.int32, piece.shape, 0) < len_ref[pair + side * pairs]
            stored[pair, :, lanes] = jnp.where(live, piece, piece[0:1, :]).astype(BF16)
        return 0

    lax.fori_loop(0, pairs, keep_live, 0)

    r_at = lax.broadcasted_iota(jnp.int32, (2 * cols, cols), 0) % cols
    c_at = lax.broadcasted_iota(jnp.int32, (2 * cols, cols), 1)
    ones_of = jnp.where(r_at // tokens == c_at // tokens, 1.0 / tokens, 0.0).astype(BF16)
    mine = (
        lax.broadcasted_iota(jnp.int32, (pairs, cols), 0) == lax.broadcasted_iota(jnp.int32, (pairs, cols), 1) % tokens
    )

    def score_block(query_cols):
        weights[0:width, 0:cols] = query_cols
        weights[width : 2 * width, cols : 2 * cols] = query_cols
        rhs = weights[...]
        for pair in range(pairs):
            similar = jnp.dot(stored[pair], rhs, preferred_element_type=F32)
            best[pair : pair + 1, :] = jnp.max(similar, axis=0, keepdims=True)
        lines = []
        for side in range(2):
            value = best[:, side * cols : (side + 1) * cols]
            high = value.astype(BF16)
            low = (value - high.astype(F32)).astype(BF16)
            summed = jnp.dot(jnp.concatenate([high, low], axis=1), ones_of, preferred_element_type=F32)
            lines.append(jnp.sum(jnp.where(mine, summed, 0.0), axis=0, keepdims=True))
        return jnp.concatenate(lines, axis=0)

    def arrived(k):
        pltpu.make_async_remote_copy(
            src_ref=own, dst_ref=held.at[k], send_sem=up_send.at[k], recv_sem=recv_sem.at[k],
            device_id={"blk": me}, device_id_type=MESH,
        ).wait_recv()

    def landed(k):
        pltpu.make_async_remote_copy(
            src_ref=outgoing.at[k], dst_ref=table.at[k], send_sem=back_send.at[k], recv_sem=back_recv.at[k],
            device_id={"blk": me}, device_id_type=MESH,
        ).wait_recv()

    table[me] = score_block(own[...])

    source_at = picked_by(ORDER, me)

    def answer(k):
        outgoing[k] = score_block(held[k])
        back(k).start()

    @pl.when(me == 0)
    def _():
        def step(t):
            @pl.when(t < last)
            def _():
                pl.semaphore_wait(barrier, 1)
                direct(t + 1).start()

            @pl.when(t >= LAG)
            def _():
                k = source_at(jnp.maximum(t - LAG, 0))
                arrived(k)
                answer(k)

        loop(0, last + LAG, step)

    @pl.when(me == 1)
    def _():
        pl.semaphore_wait(here, 1)
        climb(me, own).start()

    @pl.when(me > 0)
    def _():
        def step(t):
            k = source_at(t)
            arrived(k)

            @pl.when(k == 0)
            def _():
                direct(k).start()

            @pl.when((t == 0) & (me > 1) & (me < last))
            def _():
                pl.semaphore_wait(here, 1)

            @pl.when(((k > 0) & (k < me) & (me < last)) | (k - me > REACH + 1))
            def _():
                climb(k, held.at[k]).start()

            @pl.when((t == 0) & (me > 1) & (me < last))
            def _():
                climb(me, own).start()

            answer(k)

        loop(0, last, step)

    loop(0, me, landed)
    loop(me + 1, n, landed)

    @pl.when((me > 0) & (me < last))
    def _():
        loop(1, me, lambda k: climb(k, held.at[k]).wait_send())
        climb(me, own).wait_send()
        loop(me + REACH + 2, n, lambda k: climb(k, held.at[k]).wait_send())

    @pl.when(me == 0)
    def _():
        loop(1, n, lambda k: direct(k).wait_send())

    @pl.when(me > 0)
    def _():
        direct(jnp.int32(0)).wait_send()

        @pl.when(me - 1 > REACH)
        def _():
            direct(jnp.int32(1)).wait_send()

        loop(near, me, lambda k: direct(k).wait_send())

    loop(0, me, lambda k: back(k).wait_send())
    loop(me + 1, n, lambda k: back(k).wait_send())


def finish(slot_ref, cand_ref, table, score_ref, top_ref):
    n, _, cols = table.shape
    queries_here = cand_ref.shape[0]
    tokens = cols // queries_here
    cand = jnp.concatenate(
        [cand_ref[q : q + 1, h * 128 : (h + 1) * 128] for q in range(queries_here) for h in range(2)], axis=0
    )
    rows = gather_rows(slot_ref[...], cand // 128, cand % 128)
    query_of = lax.broadcasted_iota(jnp.int32, rows.shape, 0) // 2

    lines = table[...].reshape(2 * n, cols)
    score = gather_rows(lines, rows // tokens, query_of * tokens + rows % tokens)
    for q in range(queries_here):
        for h in range(2):
            score_ref[q : q + 1, h * 128 : (h + 1) * 128] = score[2 * q + h : 2 * q + h + 1, :]

    down = score.T
    j_at = lax.broadcasted_iota(jnp.int32, (128, 128), 0)
    k_at = lax.broadcasted_iota(jnp.int32, (128, 128), 1)
    place = lax.broadcasted_iota(jnp.int32, (16, 128), 0).astype(F32)
    spot = lax.broadcasted_iota(jnp.int32, (16, 128), 0) == lax.broadcasted_iota(jnp.int32, (16, 128), 1)
    for q in range(queries_here):
        total = jnp.zeros((16, 1), F32)
        for kh in range(2):
            k_val = score[2 * q + kh : 2 * q + kh + 1, :]
            rank = jnp.zeros((1, 128), F32)
            for jh in range(2):
                j_val = down[:, 2 * q + jh : 2 * q + jh + 1]
                if jh < kh:
                    ahead = j_val >= k_val
                elif jh > kh:
                    ahead = j_val > k_val
                else:
                    ahead = (j_val > k_val) | ((j_val == k_val) & (j_at < k_at))
                rank = rank + jnp.sum(jnp.where(ahead, 1.0, 0.0), axis=0, keepdims=True)
            total = total + jnp.sum(jnp.where(rank == place, k_val, 0.0), axis=1, keepdims=True)
        line = jnp.sum(jnp.where(spot, total, 0.0), axis=0, keepdims=True)
        top_ref[q : q + 1, :] = line[:, 0:TOPN]


def shards(n, queries, passages, lengths, slot_of, candidates):
    queries_here, tokens, width = queries.shape
    count, span, _ = passages.shape
    cols = queries_here * tokens
    vmem = pl.BlockSpec(memory_space=pltpu.VMEM)
    scores = pl.pallas_call(
        functools.partial(kernel, n),
        out_shape=jax.ShapeDtypeStruct((n, 2, cols), F32),
        in_specs=[vmem, pl.BlockSpec(memory_space=pl.ANY), pl.BlockSpec(memory_space=pltpu.SMEM)],
        out_specs=vmem,
        scratch_shapes=[
            pltpu.VMEM((width, cols), BF16),
            pltpu.VMEM((n, width, cols), BF16),
            pltpu.VMEM((count // 2, span, 2 * width), BF16),
            pltpu.VMEM((2 * width, 2 * cols), BF16),
            pltpu.VMEM((count // 2, 2 * cols), F32),
            pltpu.VMEM((n, 2, cols), F32),
            pltpu.SemaphoreType.DMA((2,)),
            pltpu.SemaphoreType.DMA((n,)),
            pltpu.SemaphoreType.DMA((n,)),
            pltpu.SemaphoreType.DMA((n,)),
            pltpu.SemaphoreType.DMA((n,)),
            pltpu.SemaphoreType.DMA((n,)),
            pltpu.SemaphoreType.REGULAR,
        ],
        compiler_params=pltpu.CompilerParams(collective_id=0, has_side_effects=True),
    )(queries, passages, lengths)
    return pl.pallas_call(
        finish,
        out_shape=(
            jax.ShapeDtypeStruct(candidates.shape, F32),
            jax.ShapeDtypeStruct((queries_here, TOPN), F32),
        ),
        in_specs=[vmem] * 3,
        out_specs=(vmem, vmem),
    )(slot_of.reshape(-1, 128), candidates, scores)


def solution(mesh):
    return jax.shard_map(
        functools.partial(shards, mesh.shape["blk"]),
        mesh=mesh,
        in_specs=(
            P(("parts", "blk", "sub", "rep"), None, None),
            P(("parts", "blk"), None, None),
            P(("parts", "blk")),
            P("parts"),
            P(("parts", "blk", "sub", "rep"), None),
        ),
        out_specs=(
            P(("parts", "blk", "sub", "rep"), None),
            P(("parts", "blk", "sub", "rep"), None),
        ),
        check_vma=False,
    )
```
